32 devices in a mesh: dp: 4 (over y, core), expert: 4 (over z), tensor: 2 (over x).
Axes of the slice: x: 2, y: 2, z: 4, core: 2. Of those that a mesh axis runs over, the one named last changes fastest.
Arguments:
- tokens: bfloat16 [96, 7168], P('expert', 'tensor'), may hold values from -6 to 6
- expert_ids: int32 [96, 8], P('expert'), may hold values from 0 to 63, all different within a row; in each aligned block of 24 rows (0 to 23, 24 to 47, ...) at most 4 rows name the same one
- gate_weights: float32 [96, 8], P('expert'), may hold values from 0.1 to 1
- w_gate: bfloat16 [64, 7168, 1024], P('expert', 'tensor', 'dp'), may hold values from -0.0625 to 0.0625
- w_up: bfloat16 [64, 7168, 1024], P('expert', 'tensor', 'dp'), may hold values from -0.0625 to 0.0625
- w_down: bfloat16 [64, 1024, 7168], P('expert', 'dp', 'tensor'), may hold values from -0.1875 to 0.1875
Outputs:
- mixed: bfloat16 [96, 7168], P('expert', 'tensor')
The draws below stay inside these ranges and needn't reach their ends.
Inputs may be any that keep to these rules, and one draw needn't show every extreme that they name: `expert_ids`: each row names 8 different experts. Among the rows of one index of the expert axis (aligned blocks of 24 rows) no expert is named more than 4 times, and in some block one expert is named exactly 4 times.
All inputs are finite; a program needn't handle non-finite values.
Results may differ from the reference program's by a relative error of at most 0.0049.
Values may be sent and summed in bfloat16 or wider, within the bound.
No kernel may reach another device: no remote copies, remote signals or barrier semaphores. Data moves between devices by JAX's collectives and lax.ppermute only.
A program may use at most 128 MiB of HBM per device.

```python
import math
import jax
import jax.numpy as jnp
import numpy as np
from jax import lax

D = 7168
FF = 1024
TOP = 8
EXPERTS = 64
T_DEV = 24
CAP = 4
TOKENS = 96
N_EXPERT = 4


def level_of(rng, dims, cuts, smallest, high):
    def one(axis_at, blocks):
        heights = jax.random.uniform(jax.random.fold_in(jax.random.fold_in(rng, 6), axis_at), (blocks,), jnp.float32, smallest / len(cuts), high / len(cuts))
        return jnp.repeat(jnp.exp(heights), dims[axis_at] // blocks).reshape((-1,) + (1,) * (len(dims) - axis_at - 1))

    gain = one(*cuts[0])
    for cut in cuts[1:]:
        gain = gain * one(*cut)
    return gain


def shared_out(key, own, number, rows, count, top, bound, slope):
    ranking = jax.random.permutation(key, count)
    packed, ordinary = shares(count, rows * top, bound, slope, True), shares(count, rows * top, bound, slope, False)
    places = jnp.arange(count)

    def named(lengths, turn):
        used = int((lengths > 0).sum())
        fixed = max(1, used // 4)
        shifted = fixed + (places - fixed + turn * (used - fixed)) % max(1, count - fixed)
        return jnp.zeros((count,), jnp.int32).at[ranking[jnp.where(places < fixed, places, shifted)]].set(jnp.asarray(lengths, jnp.int32))

    lengths = jnp.where(number % 4 == 0, named(packed, number // 4), named(ordinary, number - number // 4 - 1))
    mixed = jax.random.permutation(jax.random.fold_in(own, 3), count)
    giver, taker = mixed[0:count // 2 * 2:2], mixed[1:count // 2 * 2:2]
    room = jnp.minimum(lengths[giver] - 1, bound - lengths[taker]) // 2
    room = jnp.where((giver == ranking[0]) | (taker == ranking[0]) | (lengths[taker] == 0), 0, jnp.maximum(room, 0))
    shifted = jax.random.randint(jax.random.fold_in(own, 4), (count // 2,), 0, 1 << 20) % (room + 1)
    lengths = lengths.at[giver].add(-shifted).at[taker].add(shifted)
    members = jnp.searchsorted(jnp.cumsum(lengths), jnp.arange(rows * top), side="right").astype(jnp.int32)
    table = members.reshape(top, rows).T
    table = table[jax.random.permutation(jax.random.fold_in(own, 1), rows)]
    turn = jax.random.randint(jax.random.fold_in(own, 2), (rows, 1), 0, top)
    return jnp.take_along_axis(table, (jnp.arange(top)[None, :] + turn) % top, axis=1)


def shares(count, total, most, skew, full):
    portions = [(1 << 20) // math.isqrt(standing ** skew) + 1 for standing in range(1, count + 1)]
    largest = most if full else min(most, max(-(-total // count), total * portions[0] // sum(portions)))
    least = 1 if total - largest >= count - 1 else 0
    given, spare = [largest] + [least] * (count - 1), total - largest - least * (count - 1)
    while spare > 0:
        candidates = [i for i in range(1, count) if given[i] < largest] or [i for i in range(1, count) if given[i] < most]
        mass, remaining = sum([portions[i] for i in candidates]), spare
        for i in candidates:
            addition = min(most - given[i], max(1, remaining * portions[i] // mass), spare)
            given[i] = given[i] + addition
            spare = spare - addition
    return np.array(given)


def noise(key, shape, deviation, most, shards=(), held_as=jnp.bfloat16):
    drawn = jax.random.normal(key, shape, jnp.float32) * deviation
    if len(shards) > 0:
        drawn = level_of(key, shape, shards, -0.22, 0.18) * drawn
    return jnp.clip(drawn, min=-most, max=most).astype(held_as)


def setup_inputs(seed: int = 0) -> dict:
    key_of = jax.random.split(jax.random.key(seed), 7)
    tokens = noise(key_of[0], (TOKENS, D), 1.0, 6.0, ((0, 4), (1, 2)))
    expert_ids_keys = jax.random.split(jax.random.fold_in(key_of[1], 1), TOKENS // T_DEV)
    expert_ids_turns = jax.random.permutation(jax.random.fold_in(key_of[1], 3), TOKENS // T_DEV)
    expert_ids = jax.vmap(lambda own, number: shared_out(jax.random.fold_in(key_of[1], 2), own, number, T_DEV, EXPERTS, TOP, CAP, 2))(expert_ids_keys, expert_ids_turns).reshape((TOKENS, TOP))
    gate_weights = jnp.clip(jnp.exp(math.log(1.0) - 2.3025851 * jax.random.uniform(key_of[2], (TOKENS, TOP), jnp.float32) ** level_of(key_of[2], (TOKENS, TOP), ((0, 4),), -0.2, 0.2)), 0.1, 1.0)
    w_gate = noise(key_of[3], (EXPERTS, D, FF), D ** -0.5, 0.0625, ((0, 4), (1, 2), (2, 4)))
    w_up = noise(key_of[4], (EXPERTS, D, FF), D ** -0.5, 0.0625, ((0, 4), (1, 2), (2, 4)))
    w_down = noise(key_of[5], (EXPERTS, FF, D), FF ** -0.5, 0.1875, ((0, 4), (1, 4), (2, 2)))
    return {"tokens": tokens, "expert_ids": expert_ids, "gate_weights": gate_weights, "w_gate": w_gate, "w_up": w_up, "w_down": w_down}


def reference(tokens, expert_ids, gate_weights, w_gate, w_up, w_down):
    assignments = TOKENS * TOP
    slots_per_expert = N_EXPERT * CAP
    flat_ids = expert_ids.reshape(-1).astype(jnp.int32)
    sort_order = jnp.argsort(flat_ids, stable=True).astype(jnp.int32)
    sorted_ids = flat_ids[sort_order]
    totals = jnp.sum((flat_ids[:, None] == jnp.arange(EXPERTS, dtype=jnp.int32)[None, :]).astype(jnp.int32), axis=0)
    offsets = (jnp.cumsum(totals) - totals).astype(jnp.int32)
    slot_rank = jnp.arange(assignments, dtype=jnp.int32) - offsets[sorted_ids]
    slot_table = jnp.full((EXPERTS * slots_per_expert,), assignments, jnp.int32)
    slot_table = slot_table.at[sorted_ids * slots_per_expert + slot_rank].set(sort_order)
    slot_table = slot_table.reshape(EXPERTS, slots_per_expert)
    padded_tokens = jnp.concatenate([tokens, jnp.zeros((1, D), tokens.dtype)], axis=0)
    padded_weights = jnp.concatenate([gate_weights.reshape(-1), jnp.zeros((1,), gate_weights.dtype)])

    def one_expert(running, inputs):
        entries, gate_matrix, up_matrix, down_matrix = inputs
        token_rows = (entries // TOP).astype(jnp.int32)
        chosen = padded_tokens[token_rows]
        gate_pre = jnp.dot(chosen, gate_matrix, preferred_element_type=jnp.float32)
        up_pre = jnp.dot(chosen, up_matrix, preferred_element_type=jnp.float32)
        hidden = (jax.nn.silu(gate_pre) * up_pre).astype(jnp.bfloat16)
        expert_out = jnp.dot(hidden, down_matrix, preferred_element_type=jnp.float32)
        running = running.at[token_rows].add(expert_out * padded_weights[entries][:, None])
        return running, None

    initial = jnp.zeros((TOKENS + 1, D), jnp.float32)
    running, _ = lax.scan(one_expert, initial, (slot_table, w_gate, w_up, w_down))
    return running[:TOKENS].astype(jnp.bfloat16)
```

```python
import functools

import jax
import jax.numpy as jnp
from jax import lax
from jax.experimental import pallas as pl
from jax.experimental.pallas import tpu as pltpu
from jax.sharding import PartitionSpec as P

CAP = 4
DIRECT = 8
VMEM_BYTES = 40 * 1024 * 1024


def rotate(x, axis, shift):
    n = lax.axis_size(axis)
    return lax.ppermute(x, axis, [(i, (i + shift) % n) for i in range(n)])


def selection(code, slots):
    experts, toks = code.shape
    wide = jnp.broadcast_to(code[:, None, :], (experts, slots, toks))
    place = lax.broadcasted_iota(jnp.int32, (experts, slots, toks), 1)
    return (wide == place).reshape(experts * slots, toks)


def up_kernel(n_pieces, slots, *refs):
    codes, pieces = refs[:n_pieces], refs[n_pieces : 2 * n_pieces]
    wg_ref, wu_ref, own_ref, send_ref, rows_ref = refs[2 * n_pieces :]
    step = pl.program_id(0)
    width = rows_ref.shape[1]
    chunk = 512 if width % 512 == 0 else width

    @pl.when(step == 0)
    def _():
        picks = [selection(c[...], slots).astype(jnp.bfloat16) for c in codes]
        for at in range(0, width, chunk):
            total = None
            for pick, piece in zip(picks, pieces):
                part = jnp.dot(
                    pick, piece[:, at : at + chunk], preferred_element_type=jnp.float32
                )
                total = part if total is None else total + part
            rows_ref[:, at : at + chunk] = total.astype(jnp.bfloat16)

    lhs = rows_ref[pl.ds(pl.multiple_of(step * slots, slots), slots), :]
    gate = jnp.dot(lhs, wg_ref[0], preferred_element_type=jnp.float32)
    up = jnp.dot(lhs, wu_ref[0], preferred_element_type=jnp.float32)
    ff = gate.shape[1]
    own_ref[:, :ff] = gate
    own_ref[:, ff:] = up
    send_ref[:, :ff] = gate.astype(jnp.bfloat16)
    send_ref[:, ff:] = up.astype(jnp.bfloat16)


def up_call(codes, pieces, w_gate, w_up, first, slots):
    experts = codes[0].shape[0]
    width, ff = w_gate.shape[1], w_gate.shape[2]
    whole = lambda a: pl.BlockSpec(a.shape, lambda e: (0,) * a.ndim)
    weight = pl.BlockSpec((1, width, ff), lambda e: (e + first, 0, 0))
    out = pl.BlockSpec((slots, 2 * ff), lambda e: (e, 0))
    return pl.pallas_call(
        functools.partial(up_kernel, len(pieces), slots),
        grid=(experts,),
        in_specs=[whole(c) for c in codes] + [whole(p) for p in pieces] + [weight, weight],
        out_specs=[out, out],
        out_shape=[
            jax.ShapeDtypeStruct((experts * slots, 2 * ff), jnp.float32),
            jax.ShapeDtypeStruct((experts * slots, 2 * ff), jnp.bfloat16),
        ],
        scratch_shapes=[pltpu.VMEM((experts * slots, width), jnp.bfloat16)],
        compiler_params=pltpu.CompilerParams(
            dimension_semantics=("arbitrary",), vmem_limit_bytes=VMEM_BYTES
        ),
        cost_estimate=pl.CostEstimate(
            flops=200 * experts * width * ff, bytes_accessed=4 * experts * width * ff,
            transcendentals=0,
        ),
        name="gate_up",
    )(*codes, *pieces, w_gate, w_up)


def down_kernel(n_recv, n_out, slots, last, *refs):
    refs = list(refs)
    refs.pop(0)
    code_ref, mix_ref, own_ref = refs[:3]
    recvs = refs[3 : 3 + n_recv]
    rest = refs[3 + n_recv :]
    if last:
        wd_ref, acc_ref = rest[:2]
        outs = rest[2 : 2 + n_out]
    else:
        wd_ref = rest[0]
        outs = rest[1:2]
    hid_ref, pick_ref, scale_ref, y_ref = rest[-4:]
    step = pl.program_id(0)
    experts, ff = wd_ref.shape[0], wd_ref.shape[1]

    @pl.when(step == 0)
    def _():
        sums = own_ref[...]
        for r in recvs:
            sums = sums + r[...].astype(jnp.float32)
        gate, up = sums[:, :ff], sums[:, ff:]
        hid_ref[...] = (gate / (1.0 + jnp.exp(-gate)) * up).astype(jnp.bfloat16)
        toks = code_ref.shape[1]
        chosen = selection(code_ref[...], slots)
        mix = jnp.broadcast_to(mix_ref[...][:, None, :], (experts, slots, toks))
        mix = mix.reshape(experts * slots, toks)
        scale_ref[...] = jnp.sum(jnp.where(chosen, mix, 0.0), axis=1, keepdims=True)
        pick_ref[...] = chosen.astype(jnp.float32).T.astype(jnp.bfloat16)

    for e in range(experts):
        rows = slice(e * slots, (e + 1) * slots)
        y = jnp.dot(hid_ref[rows, :], wd_ref[e], preferred_element_type=jnp.float32)
        y_ref[rows, :] = y * scale_ref[rows, :]
    y = y_ref[...]
    high = y.astype(jnp.bfloat16)
    low = (y - high.astype(jnp.float32)).astype(jnp.bfloat16)
    pick = pick_ref[...]
    mixed = jnp.dot(pick, high, preferred_element_type=jnp.float32) + jnp.dot(
        pick, low, preferred_element_type=jnp.float32
    )
    if last:
        mixed = mixed + acc_ref[0]
        for k, out in enumerate(outs):

            @pl.when(step == k)
            def _():
                out[...] = mixed.astype(out.dtype)
    else:
        outs[0][0] = mixed


def down_call(code, mix, own, recvs, w_down, acc, first, slots, n_out, index):
    experts, toks = code.shape
    ff, width = w_down.shape[1], w_down.shape[2]
    cols = width // n_out
    last = acc is not None
    whole = lambda a: pl.BlockSpec(a.shape, lambda j, s: (0,) * a.ndim)
    if cols % 128 == 0:
        weight = pl.BlockSpec(
            (experts, ff, cols), lambda j, s: (first // experts, 0, (s[0] + j) % n_out)
        )
    else:
        w_down = w_down[first : first + experts].reshape(experts, ff, n_out, cols)
        w_down = jnp.moveaxis(w_down, 2, 0).reshape(n_out * experts, ff, cols)
        weight = pl.BlockSpec((experts, ff, cols), lambda j, s: ((s[0] + j) % n_out, 0, 0))
    acc_spec = pl.BlockSpec((1, toks, cols), lambda j, s: (j, 0, 0))
    in_specs = [whole(code), whole(mix), whole(own)] + [whole(r) for r in recvs] + [weight]
    args = [code, mix, own, *recvs, w_down]
    if last:
        in_specs.append(acc_spec)
        args.append(acc)
        out_specs = [pl.BlockSpec((toks, cols), lambda j, s: (0, 0)) for _ in range(n_out)]
        out_shape = [
            jax.ShapeDtypeStruct((toks, cols), jnp.bfloat16 if k else jnp.float32)
            for k in range(n_out)
        ]
    else:
        out_specs = acc_spec
        out_shape = jax.ShapeDtypeStruct((n_out, toks, cols), jnp.float32)
    return pl.pallas_call(
        functools.partial(down_kernel, len(recvs), n_out, slots, last),
        grid_spec=pltpu.PrefetchScalarGridSpec(
            num_scalar_prefetch=1,
            grid=(n_out,),
            in_specs=in_specs,
            out_specs=out_specs,
            scratch_shapes=[
                pltpu.VMEM((experts * slots, ff), jnp.bfloat16),
                pltpu.VMEM((toks, experts * slots), jnp.bfloat16),
                pltpu.VMEM((experts * slots, 1), jnp.float32),
                pltpu.VMEM((experts * slots, cols), jnp.float32),
            ],
        ),
        out_shape=out_shape,
        compiler_params=pltpu.CompilerParams(
            dimension_semantics=("arbitrary",), vmem_limit_bytes=VMEM_BYTES
        ),
        cost_estimate=pl.CostEstimate(
            flops=200 * experts * width * ff, bytes_accessed=2 * experts * width * ff,
            transcendentals=0,
        ),
        name="down_mix",
    )(index, *args)


def per_device(tokens, expert_ids, gate_weights, w_gate, w_up, w_down):
    n_exp = lax.axis_size("expert")
    n_dp = lax.axis_size("dp")
    n_ten = lax.axis_size("tensor")
    local = w_gate.shape[0]
    rows = tokens.shape[0]
    total = local * n_exp
    slots = CAP * n_exp
    direct = n_exp <= DIRECT

    hit = expert_ids[None, :, :] == lax.iota(jnp.int32, total)[:, None, None]
    weight = jnp.sum(jnp.where(hit, gate_weights[None], 0.0), axis=2)
    named = jnp.any(hit, axis=2)
    earlier = lax.iota(jnp.int32, rows)[:, None] < lax.iota(jnp.int32, rows)[None, :]
    rank = jnp.dot(
        named.astype(jnp.bfloat16), earlier.astype(jnp.bfloat16),
        preferred_element_type=jnp.float32,
    )
    table = jnp.stack([weight, jnp.where(named, rank, -1.0)])

    if direct:
        pieces = [tokens] + [rotate(tokens, "expert", j) for j in range(1, n_exp)]
        tables = [table] + [rotate(table, "expert", j) for j in range(1, n_exp)]
        tables = jnp.stack(tables, axis=2)
    else:
        pieces = [lax.all_gather(tokens, "expert", axis=0, tiled=True)]
        tables = lax.all_gather(table, "expert", axis=2)
    tables = lax.dynamic_slice_in_dim(tables, lax.axis_index("expert") * local, local, axis=1)
    block = lax.broadcasted_iota(jnp.int32, (local, n_exp, rows), 1)
    rank = tables[1].astype(jnp.int32)
    codes = jnp.where(rank >= 0, rank + CAP * block, -1)
    mix = tables[0].reshape(local, n_exp * rows)
    code = codes.reshape(local, n_exp * rows)
    piece_codes = [codes[:, j] for j in range(n_exp)] if direct else [code]

    groups = 2 if local % 2 == 0 and (local // 2) % 8 == 0 else 1
    size = local // groups
    owns, recvs = [], []
    for g in range(groups):
        at = slice(g * size, (g + 1) * size)
        own, send = up_call([c[at] for c in piece_codes], pieces, w_gate, w_up, g * size, slots)
        owns.append(own)
        recvs.append([rotate(send, "tensor", j) for j in range(1, n_ten)])

    me = lax.axis_index("dp").astype(jnp.int32).reshape(1)
    acc = None
    if groups == 1:
        acc = jnp.zeros((n_dp, n_exp * rows, w_down.shape[2] // n_dp), jnp.float32)
    for g in range(groups):
        at = slice(g * size, (g + 1) * size)
        acc = down_call(
            code[at], mix[at], owns[g], recvs[g], w_down, acc, g * size, slots, n_dp, me
        )

    part = acc[0]
    for k in range(1, n_dp):
        part = part + rotate(acc[k], "dp", k).astype(jnp.float32)
    if direct:
        mine = part[:rows]
        for j in range(1, n_exp):
            back = part[j * rows : (j + 1) * rows].astype(jnp.bfloat16)
            mine = mine + rotate(back, "expert", -j).astype(jnp.float32)
    else:
        mine = lax.psum_scatter(part, "expert", scatter_dimension=0, tiled=True)
    return lax.all_gather(mine.astype(jnp.bfloat16), "dp", axis=1, tiled=True)


def solution(mesh):
    in_specs = (
        P("expert", "tensor"),
        P("expert", None),
        P("expert", None),
        P("expert", "tensor", "dp"),
        P("expert", "tensor", "dp"),
        P("expert", "dp", "tensor"),
    )
    out_specs = P("expert", "tensor")
    return jax.shard_map(
        per_device, mesh=mesh, in_specs=in_specs, out_specs=out_specs, check_vma=False
    )
```

```python
import functools

import jax
import jax.numpy as jnp
from jax import lax
from jax.experimental import pallas as pl
from jax.experimental.pallas import tpu as pltpu
from jax.sharding import PartitionSpec as P

CAP = 4
DIRECT = 8
VMEM_BYTES = 40 * 1024 * 1024


def rotate(x, axis, shift):
    n = lax.axis_size(axis)
    return lax.ppermute(x, axis, [(i, (i + shift) % n) for i in range(n)])


def selection(code, slots):
    experts, toks = code.shape
    wide = jnp.broadcast_to(code[:, None, :], (experts, slots, toks))
    place = lax.broadcasted_iota(jnp.int32, (experts, slots, toks), 1)
    return (wide == place).reshape(experts * slots, toks)


def up_kernel(n_pieces, slots, *refs):
    codes, pieces = refs[:n_pieces], refs[n_pieces : 2 * n_pieces]
    wg_ref, wu_ref, own_ref, send_ref, rows_ref = refs[2 * n_pieces :]
    step = pl.program_id(0)
    width = rows_ref.shape[1]
    chunk = 512 if width % 512 == 0 else width

    @pl.when(step == 0)
    def _():
        picks = [selection(c[...], slots).astype(jnp.bfloat16) for c in codes]
        for at in range(0, width, chunk):
            total = None
            for pick, piece in zip(picks, pieces):
                part = jnp.dot(
                    pick, piece[:, at : at + chunk], preferred_element_type=jnp.float32
                )
                total = part if total is None else total + part
            rows_ref[:, at : at + chunk] = total.astype(jnp.bfloat16)

    lhs = rows_ref[pl.ds(pl.multiple_of(step * slots, slots), slots), :]
    gate = jnp.dot(lhs, wg_ref[0], preferred_element_type=jnp.float32)
    up = jnp.dot(lhs, wu_ref[0], preferred_element_type=jnp.float32)
    ff = gate.shape[1]
    own_ref[:, :ff] = gate
    own_ref[:, ff:] = up
    send_ref[:, :ff] = gate.astype(jnp.bfloat16)
    send_ref[:, ff:] = up.astype(jnp.bfloat16)


def up_call(codes, pieces, w_gate, w_up, first, slots):
    experts = codes[0].shape[0]
    width, ff = w_gate.shape[1], w_gate.shape[2]
    whole = lambda a: pl.BlockSpec(a.shape, lambda e: (0,) * a.ndim)
    weight = pl.BlockSpec((1, width, ff), lambda e: (e + first, 0, 0))
    out = pl.BlockSpec((slots, 2 * ff), lambda e: (e, 0))
    return pl.pallas_call(
        functools.partial(up_kernel, len(pieces), slots),
        grid=(experts,),
        in_specs=[whole(c) for c in codes] + [whole(p) for p in pieces] + [weight, weight],
        out_specs=[out, out],
        out_shape=[
            jax.ShapeDtypeStruct((experts * slots, 2 * ff), jnp.float32),
            jax.ShapeDtypeStruct((experts * slots, 2 * ff), jnp.bfloat16),
        ],
        scratch_shapes=[pltpu.VMEM((experts * slots, width), jnp.bfloat16)],
        compiler_params=pltpu.CompilerParams(
            dimension_semantics=("arbitrary",), vmem_limit_bytes=VMEM_BYTES
        ),
        cost_estimate=pl.CostEstimate(
            flops=200 * experts * width * ff, bytes_accessed=4 * experts * width * ff,
            transcendentals=0,
        ),
        name="gate_up",
    )(*codes, *pieces, w_gate, w_up)


def down_kernel(n_recv, n_out, slots, last, *refs):
    refs = list(refs)
    refs.pop(0)
    code_ref, mix_ref, own_ref = refs[:3]
    recvs = refs[3 : 3 + n_recv]
    rest = refs[3 + n_recv :]
    if last:
        wd_ref, acc_ref = rest[:2]
        outs = rest[2 : 2 + n_out]
    else:
        wd_ref = rest[0]
        outs = rest[1:2]
    hid_ref, pick_ref, scale_ref, y_ref = rest[-4:]
    step = pl.program_id(0)
    experts, ff = wd_ref.shape[0], wd_ref.shape[1]

    @pl.when(step == 0)
    def _():
        sums = own_ref[...]
        for r in recvs:
            sums = sums + r[...].astype(jnp.float32)
        gate, up = sums[:, :ff], sums[:, ff:]
        hid_ref[...] = (gate / (1.0 + jnp.exp(-gate)) * up).astype(jnp.bfloat16)
        toks = code_ref.shape[1]
        chosen = selection(code_ref[...], slots)
        mix = jnp.broadcast_to(mix_ref[...][:, None, :], (experts, slots, toks))
        mix = mix.reshape(experts * slots, toks)
        scale_ref[...] = jnp.sum(jnp.where(chosen, mix, 0.0), axis=1, keepdims=True)
        pick_ref[...] = chosen.astype(jnp.float32).T.astype(jnp.bfloat16)

    for e in range(experts):
        rows = slice(e * slots, (e + 1) * slots)
        y = jnp.dot(hid_ref[rows, :], wd_ref[e], preferred_element_type=jnp.float32)
        y_ref[rows, :] = y * scale_ref[rows, :]
    y = y_ref[...]
    high = y.astype(jnp.bfloat16)
    low = (y - high.astype(jnp.float32)).astype(jnp.bfloat16)
    pick = pick_ref[...]
    mixed = jnp.dot(pick, high, preferred_element_type=jnp.float32) + jnp.dot(
        pick, low, preferred_element_type=jnp.float32
    )
    if last:
        mixed = mixed + acc_ref[0]
        for k, out in enumerate(outs):

            @pl.when(step == k)
            def _():
                out[...] = mixed.astype(out.dtype)
    else:
        outs[0][0] = mixed


def down_call(code, mix, own, recvs, w_down, acc, first, slots, n_out, index):
    experts, toks = code.shape
    ff, width = w_down.shape[1], w_down.shape[2]
    cols = width // n_out
    last = acc is not None
    whole = lambda a: pl.BlockSpec(a.shape, lambda j, s: (0,) * a.ndim)
    if cols % 128 == 0:
        weight = pl.BlockSpec(
            (experts, ff, cols), lambda j, s: (first // experts, 0, (s[0] + j) % n_out)
        )
    else:
        w_down = w_down[first : first + experts].reshape(experts, ff, n_out, cols)
        w_down = jnp.moveaxis(w_down, 2, 0).reshape(n_out * experts, ff, cols)
        weight = pl.BlockSpec((experts, ff, cols), lambda j, s: ((s[0] + j) % n_out, 0, 0))
    acc_spec = pl.BlockSpec((1, toks, cols), lambda j, s: (j, 0, 0))
    in_specs = [whole(code), whole(mix), whole(own)] + [whole(r) for r in recvs] + [weight]
    args = [code, mix, own, *recvs, w_down]
    if last:
        in_specs.append(acc_spec)
        args.append(acc)
        out_specs = [pl.BlockSpec((toks, cols), lambda j, s: (0, 0)) for _ in range(n_out)]
        out_shape = [
            jax.ShapeDtypeStruct((toks, cols), jnp.bfloat16 if k else jnp.float32)
            for k in range(n_out)
        ]
    else:
        out_specs = acc_spec
        out_shape = jax.ShapeDtypeStruct((n_out, toks, cols), jnp.float32)
    return pl.pallas_call(
        functools.partial(down_kernel, len(recvs), n_out, slots, last),
        grid_spec=pltpu.PrefetchScalarGridSpec(
            num_scalar_prefetch=1,
            grid=(n_out,),
            in_specs=in_specs,
            out_specs=out_specs,
            scratch_shapes=[
                pltpu.VMEM((experts * slots, ff), jnp.bfloat16),
                pltpu.VMEM((toks, experts * slots), jnp.bfloat16),
                pltpu.VMEM((experts * slots, 1), jnp.float32),
                pltpu.VMEM((experts * slots, cols), jnp.float32),
            ],
        ),
        out_shape=out_shape,
        compiler_params=pltpu.CompilerParams(
            dimension_semantics=("arbitrary",), vmem_limit_bytes=VMEM_BYTES
        ),
        cost_estimate=pl.CostEstimate(
            flops=200 * experts * width * ff, bytes_accessed=2 * experts * width * ff,
            transcendentals=0,
        ),
        name="down_mix",
    )(index, *args)


def per_device(tokens, expert_ids, gate_weights, w_gate, w_up, w_down):
    n_exp = lax.axis_size("expert")
    n_dp = lax.axis_size("dp")
    n_ten = lax.axis_size("tensor")
    local = w_gate.shape[0]
    rows = tokens.shape[0]
    total = local * n_exp
    slots = CAP * n_exp
    direct = n_exp <= DIRECT

    hit = expert_ids[None, :, :] == lax.iota(jnp.int32, total)[:, None, None]
    weight = jnp.sum(jnp.where(hit, gate_weights[None], 0.0), axis=2)
    named = jnp.any(hit, axis=2)
    earlier = lax.iota(jnp.int32, rows)[:, None] < lax.iota(jnp.int32, rows)[None, :]
    rank = jnp.dot(
        named.astype(jnp.bfloat16), earlier.astype(jnp.bfloat16),
        preferred_element_type=jnp.float32,
    )
    table = jnp.stack([weight, jnp.where(named, rank, -1.0)])

    if direct:
        pieces = [tokens] + [rotate(tokens, "expert", j) for j in range(1, n_exp)]
        if n_exp > 1:
            table, pieces[1] = lax.optimization_barrier((table, pieces[1]))
        tables = [table] + [rotate(table, "expert", j) for j in range(1, n_exp)]
        tables = jnp.stack(tables, axis=2)
    else:
        pieces = [lax.all_gather(tokens, "expert", axis=0, tiled=True)]
        tables = lax.all_gather(table, "expert", axis=2)
    tables = lax.dynamic_slice_in_dim(tables, lax.axis_index("expert") * local, local, axis=1)
    block = lax.broadcasted_iota(jnp.int32, (local, n_exp, rows), 1)
    rank = tables[1].astype(jnp.int32)
    codes = jnp.where(rank >= 0, rank + CAP * block, -1)
    mix = tables[0].reshape(local, n_exp * rows)
    code = codes.reshape(local, n_exp * rows)
    piece_codes = [codes[:, j] for j in range(n_exp)] if direct else [code]

    groups = 2 if local % 2 == 0 and (local // 2) % 8 == 0 else 1
    size = local // groups
    owns, recvs = [], []
    for g in range(groups):
        at = slice(g * size, (g + 1) * size)
        own, send = up_call([c[at] for c in piece_codes], pieces, w_gate, w_up, g * size, slots)
        owns.append(own)
        recvs.append([rotate(send, "tensor", j) for j in range(1, n_ten)])

    me = lax.axis_index("dp").astype(jnp.int32).reshape(1)
    acc = None
    if groups == 1:
        acc = jnp.zeros((n_dp, n_exp * rows, w_down.shape[2] // n_dp), jnp.float32)
    for g in range(groups):
        at = slice(g * size, (g + 1) * size)
        acc = down_call(
            code[at], mix[at], owns[g], recvs[g], w_down, acc, g * size, slots, n_dp, me
        )

    part = acc[0]
    for k in range(1, n_dp):
        part = part + rotate(acc[k], "dp", k).astype(jnp.float32)
    if direct:
        mine = part[:rows]
        for j in range(1, n_exp):
            back = part[j * rows : (j + 1) * rows].astype(jnp.bfloat16)
            mine = mine + rotate(back, "expert", -j).astype(jnp.float32)
    else:
        mine = lax.psum_scatter(part, "expert", scatter_dimension=0, tiled=True)
    return lax.all_gather(mine.astype(jnp.bfloat16), "dp", axis=1, tiled=True)


def solution(mesh):
    in_specs = (
        P("expert", "tensor"),
        P("expert", None),
        P("expert", None),
        P("expert", "tensor", "dp"),
        P("expert", "tensor", "dp"),
        P("expert", "dp", "tensor"),
    )
    out_specs = P("expert", "tensor")
    return jax.shard_map(
        per_device, mesh=mesh, in_specs=in_specs, out_specs=out_specs, check_vma=False
    )
```
